32 devices in a mesh: row: 4 (over x, core), col: 8 (over z, y).
Axes of the slice: x: 2, y: 2, z: 4, core: 2. Of those that a mesh axis runs over, the one named last changes fastest.
Arguments:
- panel: bfloat16 [32768, 512], P('row', 'col'), may hold values from -0.03125 to 0.03125
- pheno: bfloat16 [32768, 2048], P('row', 'col'), may hold values from -48 to 48
- kin_values: float32 [512], replicated, may hold values from 0.1 to 10
- trait_values: float32 [128], replicated, may hold values from 0.1 to 10
- trait_basis: float32 [128, 128], replicated, may hold values from -0.5 to 0.5
Outputs:
- coeffs: float32 [512, 2048], P('row', 'col')
- genetic: bfloat16 [32768, 2048], P('row', 'col')
The draws below stay inside these ranges and needn't reach their ends.
All inputs are finite; a program needn't handle non-finite values.
Results may differ from the reference program's by a relative error of at most 0.0049.
Values may be sent and summed in bfloat16 or wider, within the bound.
A program may use at most 64 MiB of HBM per device.

```python
import math
import jax
import jax.numpy as jnp
from jax import lax

PANEL = 512
TRAITS = 128
NIND = 32768
SETS = 16


def block_levels(key, dims, pieces, smallest, high):
    gain = 1.0
    for dim, blocks in pieces:
        draws = jax.random.uniform(jax.random.fold_in(jax.random.fold_in(key, 6), dim), (blocks,), jnp.float32, smallest / len(pieces), high / len(pieces))
        gain = gain * jnp.repeat(jnp.exp(draws), dims[dim] // blocks).reshape((-1,) + (1,) * (len(dims) - 1 - dim))
    return gain


def gaussian(rng, shape, width, bound, cuts=(), kind=jnp.bfloat16):
    values = jax.random.normal(rng, shape, jnp.float32) * width
    if len(cuts) > 0:
        values = block_levels(rng, shape, cuts, -0.22, 0.18) * values
    return jnp.clip(values, min=-bound, max=bound).astype(kind)


def setup_inputs(seed: int = 0) -> dict:
    key_list = jax.random.split(jax.random.key(seed), 6)
    panel = gaussian(key_list[0], (NIND, PANEL), NIND ** -0.5, 0.03125, ((0, 4), (1, 8)))
    pheno = gaussian(key_list[1], (NIND, TRAITS * SETS), 8.0, 48.0, ((0, 4), (1, 8)))
    kin_values = jnp.clip(jnp.exp(jax.random.uniform(key_list[2], (PANEL,), jnp.float32, math.log(0.1), math.log(10.0))), 0.1, 10.0)
    trait_values = jnp.clip(jnp.exp(jax.random.uniform(key_list[3], (TRAITS,), jnp.float32, math.log(0.1), math.log(10.0))), 0.1, 10.0)
    trait_basis = gaussian(key_list[4], (TRAITS, TRAITS), TRAITS ** -0.5, 0.5, (), jnp.float32)
    return {"panel": panel, "pheno": pheno, "kin_values": kin_values, "trait_values": trait_values, "trait_basis": trait_basis}


def reference(panel, pheno, kin_values, trait_values, trait_basis):
    projected = jnp.dot(panel.T, pheno, preferred_element_type=jnp.float32)
    layered = projected.reshape(PANEL, TRAITS, SETS)
    rotated = jnp.einsum("pts,tj->psj", layered, trait_basis, precision=lax.Precision.HIGHEST)
    product = kin_values[:, None] * trait_values[None, :]
    scaled = rotated * (product / (product + 1.0))[:, None, :]
    unrotated = jnp.einsum("psj,tj->pts", scaled, trait_basis, precision=lax.Precision.HIGHEST)
    coeffs = unrotated.reshape(PANEL, TRAITS * SETS)
    genetic = jnp.dot(panel, coeffs.astype(jnp.bfloat16), preferred_element_type=jnp.float32)
    return coeffs, genetic.astype(jnp.bfloat16)
```

```python
import functools

import jax
import jax.numpy as jnp
from jax import lax
from jax.experimental import pallas as pl
from jax.experimental.pallas import tpu as pltpu
from jax.sharding import PartitionSpec as P

LANES = 128
PIECES = 4
MESH = pl.DeviceIdType.MESH
HIGH = lax.Precision.HIGHEST


def gather_rotate(
    rows, cols, q, pheno, basis, basis_t, kin, trait,
    g_out, c_out, coeffs_out,
    g, ph, pht, acc, part_f, part, rparts, sb, rb, ob, crow, ct,
    load_sem, send_sem, recv_sem, out_sem, rs_send, rs_recv, a1_send, a1_recv, a2_send, a2_recv, ag_send, ag_recv,
):
    me_r, me_c = lax.axis_index("row"), lax.axis_index("col")
    lines = cols // 2
    z, y = me_c // 2, lax.rem(me_c, 2)
    other = me_c + 1 - 2 * y
    half_ind = q.shape[0]
    piece = half_ind // PIECES
    columns = pheno.shape[1]
    traits = basis.shape[0]
    sets = columns * cols // traits
    t_here = traits // cols
    width = LANES // 2

    own_load = pltpu.make_async_copy(q, g.at[me_c], load_sem.at[0])
    own_load.start()
    ph_load = pltpu.make_async_copy(pheno, ph, load_sem.at[1])
    ph_load.start()

    barrier = pltpu.get_barrier_semaphore()
    for d in range(1, cols):
        pl.semaphore_signal(barrier, inc=1, device_id=(me_r, lax.rem(me_c + d, cols)), device_id_type=MESH)
    for d in range(1, rows):
        pl.semaphore_signal(barrier, inc=1, device_id=(lax.rem(me_r + d, rows), me_c), device_id_type=MESH)
    pl.semaphore_wait(barrier, cols + rows - 2)

    def hop(way, block, j):
        target = (jnp.minimum(me_c + 2, cols - 2 + y), jnp.maximum(me_c - 2, y), other)[way]
        here = g.at[block, pl.ds(j * piece, piece)]
        return pltpu.make_async_remote_copy(
            src_ref=here, dst_ref=here,
            send_sem=send_sem.at[way, block, j], recv_sem=recv_sem.at[block, j],
            device_id=(me_r, target), device_id_type=MESH,
        )

    def arrived(block, j):
        hop(2, block, j).wait_recv()

    up, down = z < lines - 1, z > 0
    late = PIECES // 2

    def line_sends(block, j, act):
        @pl.when(up)
        def _():
            act(hop(0, block, j))

        @pl.when(down)
        def _():
            act(hop(1, block, j))

    own_load.wait()
    for j in range(PIECES):
        line_sends(me_c, j, lambda h: h.start())
        hop(2, me_c, j).start()

    ph_load.wait()
    tile = 256

    def turn(i, _):
        for h in range(2):
            at = pl.multiple_of(h * half_ind + i * tile, tile)
            pht[h * columns:(h + 1) * columns, pl.ds(pl.multiple_of(i * tile, tile), tile)] = ph[pl.ds(at, tile), :].T
        return 0

    lax.fori_loop(0, half_ind // tile, turn, 0)

    def project(pair):
        mine, theirs = 2 * pair + y, 2 * pair + 1 - y
        for b in (2 * pair, 2 * pair + 1):
            pltpu.make_async_copy(g.at[b], g_out.at[b], out_sem.at[b]).start()
        acc[...] = jnp.zeros_like(acc)
        step = 1024

        def add(i, _):
            at = pl.ds(pl.multiple_of(i * step, step), step)
            rhs = jnp.concatenate([g[2 * pair, at, :], g[2 * pair + 1, at, :]], axis=1)
            acc[...] += jnp.dot(pht[:, at], rhs, preferred_element_type=jnp.float32)
            return 0

        lax.fori_loop(0, half_ind // step, add, 0)
        lane = lax.broadcasted_iota(jnp.int32, (columns, LANES), 1)
        low = lane < width
        top, bottom = acc[:columns, :], acc[columns:, :]
        first = top[:, :LANES] + pltpu.roll(bottom[:, :LANES], width, 1)
        second = pltpu.roll(top[:, LANES:], width, 1) + bottom[:, LANES:]
        part_f[...] = jnp.where(low, first, second)
        for s in range(sets):
            part[pair, s * t_here:(s + 1) * t_here, :] = part_f[pl.ds(s, t_here, stride=sets), :].astype(jnp.bfloat16)

        @pl.when(pair != me_r)
        def _():
            reduce_copy(pair).start()

    def reduce_copy(pair):
        return pltpu.make_async_remote_copy(
            src_ref=part.at[pair], dst_ref=rparts.at[me_r],
            send_sem=rs_send.at[pair], recv_sem=rs_recv.at[me_r],
            device_id=(pair, me_c), device_id_type=MESH,
        )

    def wait_theirs(pair):
        for j in range(PIECES):
            arrived(2 * pair + 1 - y, j)

    def around(s, fn):
        @pl.when(z - s >= 0)
        def _():
            fn(z - s)

        @pl.when(z + s < lines)
        def _():
            fn(z + s)

    def late_round(pair):
        wait_theirs(pair)
        project(pair)

    for s in range(1, lines):
        for j in range(PIECES):
            skip = s == 1 and j >= late

            @pl.when(z - s >= 0)
            def _():
                b = me_c - 2 * s
                arrived(b, j)

                @pl.when(up)
                def _():
                    hop(0, b, j).start()

                if not skip:
                    hop(2, b, j).start()

            @pl.when(z + s < lines)
            def _():
                b = me_c + 2 * s
                arrived(b, j)

                @pl.when(down)
                def _():
                    hop(1, b, j).start()

                if not skip:
                    hop(2, b, j).start()

        if s == 1:
            wait_theirs(z)
            project(z)
    for j in range(late, PIECES):
        line_sends(other, j, lambda h: h.start())
    for s in list(range(2, lines)) + [1]:
        around(s, late_round)

    total = part[me_r].astype(jnp.float32)
    for d in range(1, rows):
        src = lax.rem(me_r + d, rows)
        pltpu.make_async_remote_copy(
            src_ref=part.at[src], dst_ref=rparts.at[src], send_sem=rs_send.at[src], recv_sem=rs_recv.at[src],
            device_id=(src, me_c), device_id_type=MESH,
        ).wait_recv()
        total = total + rparts[src].astype(jnp.float32)
    sb[...] = total.astype(jnp.bfloat16).reshape(sb.shape)

    def trade1(peer, slot):
        return pltpu.make_async_remote_copy(
            src_ref=sb.at[peer], dst_ref=rb.at[slot], send_sem=a1_send.at[peer], recv_sem=a1_recv.at[slot],
            device_id=(me_r, peer), device_id_type=MESH,
        )

    def trade2(peer, slot):
        return pltpu.make_async_remote_copy(
            src_ref=ob.at[peer], dst_ref=crow.at[me_r, slot], send_sem=a2_send.at[peer], recv_sem=a2_recv.at[slot],
            device_id=(me_r, peer), device_id_type=MESH,
        )

    def share(peer, slot):
        return pltpu.make_async_remote_copy(
            src_ref=crow.at[me_r], dst_ref=crow.at[slot], send_sem=ag_send.at[peer], recv_sem=ag_recv.at[slot],
            device_id=(peer, me_c), device_id_type=MESH,
        )

    col_peers = [lax.rem(me_c + d, cols) for d in range(1, cols)]
    row_peers = [lax.rem(me_r + d, rows) for d in range(1, rows)]
    for p in col_peers:
        trade1(p, me_c).start()
    rb[me_c] = sb[me_c]
    product = kin[pl.ds(me_r, 1), :] * trait[...]
    weight = product / (product + 1.0)
    for p in col_peers:
        trade1(p, p).wait_recv()
    s_here = sets // cols
    got = jnp.concatenate(
        [rb[:, s * t_here:(s + 1) * t_here, :].astype(jnp.float32).reshape(traits, LANES) for s in range(s_here)], axis=1
    )
    rotated = jnp.dot(basis_t[...], got, precision=HIGH, preferred_element_type=jnp.float32)
    scaled = rotated * jnp.concatenate([weight] * s_here, axis=1)
    back = jnp.dot(basis[...], scaled, precision=HIGH, preferred_element_type=jnp.float32)
    for s in range(s_here):
        ob[:, s * t_here:(s + 1) * t_here, :] = (
            back[:, s * LANES:(s + 1) * LANES].reshape(cols, t_here, LANES).astype(jnp.bfloat16)
        )
    for p in col_peers:
        trade2(p, me_c).start()
    crow[me_r, me_c] = ob[me_c]
    for p in col_peers:
        trade2(p, p).wait_recv()
    for p in row_peers:
        share(p, me_r).start()

    def place(r):
        for s in range(sets):
            part_s = crow[r, s // s_here, (s % s_here) * t_here:(s % s_here + 1) * t_here, :]
            ct[pl.ds(s, t_here, stride=sets), :] = part_s.astype(jnp.float32)
        turned = ct[...].T
        c_out[pl.ds(pl.multiple_of(r * LANES, LANES), LANES), :] = turned.astype(jnp.bfloat16)
        return turned

    coeffs_out[...] = place(me_r)
    for p in row_peers:
        share(p, p).wait_recv()
        place(p)

    for j in range(PIECES):
        line_sends(me_c, j, lambda h: h.wait_send())
        hop(2, me_c, j).wait_send()
        if j >= late:
            line_sends(other, j, lambda h: h.wait_send())
        for s in range(1, lines):
            skip = s == 1 and j >= late

            @pl.when(z - s >= 0)
            def _():
                @pl.when(up)
                def _():
                    hop(0, me_c - 2 * s, j).wait_send()

                if not skip:
                    hop(2, me_c - 2 * s, j).wait_send()

            @pl.when(z + s < lines)
            def _():
                @pl.when(down)
                def _():
                    hop(1, me_c + 2 * s, j).wait_send()

                if not skip:
                    hop(2, me_c + 2 * s, j).wait_send()

    for p in row_peers:
        reduce_copy(p).wait_send()
        share(p, me_r).wait_send()
    for p in col_peers:
        trade1(p, me_c).wait_send()
        trade2(p, me_c).wait_send()
    for b in range(cols):
        pltpu.make_async_copy(g.at[b], g_out.at[b], out_sem.at[b]).wait()


def predict(g, c, out, wide):
    blocks = g.shape[0]
    width = LANES // 2
    columns = c.shape[1]

    @pl.when(pl.program_id(0) == 0)
    def _():
        wide[...] = jnp.zeros_like(wide)
        for k in range(blocks):
            rows = c[k * width:(k + 1) * width, :]
            wide[k * LANES:k * LANES + width, :columns] = rows
            wide[k * LANES + width:(k + 1) * LANES, columns:] = rows

    lhs = jnp.concatenate([g[k] for k in range(blocks)], axis=1)
    res = jnp.dot(lhs, wide[...], preferred_element_type=jnp.float32).astype(jnp.bfloat16)
    out[0] = res[:, :columns]
    out[1] = res[:, columns:]


def fused(panel, pheno, kin_values, trait_values, trait_basis):
    rows, cols = lax.axis_size("row"), lax.axis_size("col")
    ind, columns = pheno.shape
    half = ind // 2
    traits = trait_basis.shape[0]
    sets = columns * cols // traits
    share = kin_values.shape[0] // rows
    q = jnp.concatenate([panel[:half], panel[half:]], axis=1)
    bf, f32 = jnp.bfloat16, jnp.float32
    hbm = pl.BlockSpec(memory_space=pltpu.HBM)
    vmem = pl.BlockSpec(memory_space=pltpu.VMEM)
    lot = columns // cols
    dma = pltpu.SemaphoreType.DMA
    g, c, coeffs = pl.pallas_call(
        functools.partial(gather_rotate, rows, cols),
        out_shape=(
            jax.ShapeDtypeStruct((cols, half, LANES), bf),
            jax.ShapeDtypeStruct((rows * share, columns), bf),
            jax.ShapeDtypeStruct((share, columns), f32),
        ),
        in_specs=[hbm, hbm, vmem, vmem, vmem, vmem],
        out_specs=(hbm, vmem, vmem),
        scratch_shapes=[
            pltpu.VMEM((cols, half, LANES), bf),
            pltpu.VMEM((ind, columns), bf),
            pltpu.VMEM((2 * columns, half), bf),
            pltpu.VMEM((2 * columns, 2 * LANES), f32),
            pltpu.VMEM((columns, LANES), f32),
            pltpu.VMEM((rows, columns, LANES), bf),
            pltpu.VMEM((rows, columns, LANES), bf),
            pltpu.VMEM((cols, lot, LANES), bf),
            pltpu.VMEM((cols, lot, LANES), bf),
            pltpu.VMEM((cols, lot, LANES), bf),
            pltpu.VMEM((rows, cols, lot, LANES), bf),
            pltpu.VMEM((columns, LANES), f32),
            dma((2,)), dma((3, cols, PIECES)), dma((cols, PIECES)), dma((cols,)),
            dma((rows,)), dma((rows,)), dma((cols,)), dma((cols,)), dma((cols,)), dma((cols,)),
            dma((rows,)), dma((rows,)),
        ],
        compiler_params=pltpu.CompilerParams(
            collective_id=0, has_side_effects=True, vmem_limit_bytes=40 * 1024 * 1024
        ),
    )(q, pheno, trait_basis, trait_basis.T, kin_values.reshape(rows, share), trait_values[:, None])
    tile = 512
    genetic = pl.pallas_call(
        predict,
        out_shape=jax.ShapeDtypeStruct((2, half, columns), bf),
        grid=(half // tile,),
        in_specs=[
            pl.BlockSpec((cols, tile, LANES), lambda i: (0, i, 0)),
            pl.BlockSpec((rows * share, columns), lambda i: (0, 0)),
        ],
        out_specs=pl.BlockSpec((2, tile, columns), lambda i: (0, i, 0)),
        scratch_shapes=[pltpu.VMEM((cols * LANES, 2 * columns), bf)],
    )(g, c)
    return coeffs, genetic.reshape(ind, columns)


def local(panel, pheno, kin_values, trait_values, trait_basis):
    rows, cols = lax.axis_size("row"), lax.axis_size("col")
    eigen = kin_values.shape[0]
    if 2 * panel.shape[1] == LANES and eigen // rows == LANES and trait_basis.shape[0] // cols == 16:
        return fused(panel, pheno, kin_values, trait_values, trait_basis)
    return plain(panel, pheno, kin_values, trait_values, trait_basis)


def plain(panel, pheno, kin_values, trait_values, trait_basis):
    col_count = lax.axis_size("col")
    columns = pheno.shape[1]
    traits = trait_basis.shape[0]
    traits_here = traits // col_count
    set_count = columns // traits_here
    sets_dev = set_count // col_count
    whole_panel = lax.all_gather(panel, "col", axis=1, tiled=True)
    partial_value = lax.dot_general(
        whole_panel, pheno, (((0,), (0,)), ((), ())), preferred_element_type=jnp.float32
    )
    summed = lax.psum_scatter(partial_value, "row", scatter_dimension=0, tiled=True)
    first_row = lax.axis_index("row") * summed.shape[0]
    share_rows = summed.shape[0]
    by_trait = summed.reshape(share_rows, traits_here, set_count).transpose(0, 2, 1)
    by_trait = by_trait.reshape(share_rows, set_count * traits_here)
    grouped = lax.all_to_all(by_trait, "col", split_axis=1, concat_axis=1, tiled=True)
    grouped = grouped.reshape(share_rows, col_count, sets_dev, traits_here).transpose(0, 2, 1, 3)
    grouped = grouped.reshape(share_rows, sets_dev, traits)
    rotated = jnp.einsum("rst,tj->rsj", grouped, trait_basis, precision=HIGH)
    kin_rows = lax.dynamic_slice_in_dim(kin_values, first_row, share_rows, 0)
    product = kin_rows[:, None] * trait_values[None, :]
    scaled = rotated * (product / (product + 1.0))[:, None, :]
    unrotated = jnp.einsum("rsj,tj->rst", scaled, trait_basis, precision=HIGH)
    outgoing = unrotated.reshape(share_rows, sets_dev, col_count, traits_here).transpose(0, 2, 1, 3)
    outgoing = outgoing.reshape(share_rows, col_count * sets_dev * traits_here)
    returned = lax.all_to_all(outgoing, "col", split_axis=1, concat_axis=1, tiled=True)
    coeffs = returned.reshape(share_rows, set_count, traits_here).transpose(0, 2, 1)
    coeffs = coeffs.reshape(share_rows, columns)
    coeffs_low = lax.all_gather(coeffs.astype(jnp.bfloat16), "row", axis=0, tiled=True)
    genetic = jnp.dot(whole_panel, coeffs_low, preferred_element_type=jnp.float32)
    return (coeffs, genetic.astype(jnp.bfloat16))


def solution(mesh):
    return jax.shard_map(
        local,
        mesh=mesh,
        in_specs=(P("row", "col"), P("row", "col"), P(), P(), P()),
        out_specs=(P("row", "col"), P("row", "col")),
        check_vma=False,
    )
```

```python
import functools

import jax
import jax.numpy as jnp
from jax import lax
from jax.experimental import pallas as pl
from jax.experimental.pallas import tpu as pltpu
from jax.sharding import PartitionSpec as P

LANES = 128
PIECES = 4
MESH = pl.DeviceIdType.MESH
HIGH = lax.Precision.HIGHEST


def gather_rotate(
    rows, cols, q, pheno, basis, kin, trait,
    gen_out, coeffs_out,
    w_out, c_out, held, gen_sem, g, ph, acc, part_f, part, rparts, sb, rb, ob, crow, ct,
    load_sem, send_sem, recv_sem, rs_send, rs_recv, a1_send, a1_recv, a2_send, a2_recv, ag_send, ag_recv,
):
    me_r, me_c = lax.axis_index("row"), lax.axis_index("col")
    lines = cols // 2
    z, y = me_c // 2, lax.rem(me_c, 2)
    other = me_c + 1 - 2 * y
    width, people = q.shape
    piece = width // PIECES
    columns = pheno.shape[1]
    traits = basis.shape[0]
    sets = columns * cols // traits
    t_here = traits // cols

    own_load = pltpu.make_async_copy(q, g.at[me_c], load_sem.at[0])
    own_load.start()
    ph_load = pltpu.make_async_copy(pheno, ph, load_sem.at[1])
    ph_load.start()

    barrier = pltpu.get_barrier_semaphore()
    for d in range(1, cols):
        pl.semaphore_signal(barrier, inc=1, device_id=(me_r, lax.rem(me_c + d, cols)), device_id_type=MESH)
    for d in range(1, rows):
        pl.semaphore_signal(barrier, inc=1, device_id=(lax.rem(me_r + d, rows), me_c), device_id_type=MESH)
    pl.semaphore_wait(barrier, cols + rows - 2)

    def hop(way, block, j):
        target = (jnp.minimum(me_c + 2, cols - 2 + y), jnp.maximum(me_c - 2, y), other)[way]
        here = g.at[block, pl.ds(j * piece, piece)]
        return pltpu.make_async_remote_copy(
            src_ref=here, dst_ref=here,
            send_sem=send_sem.at[way, block, j], recv_sem=recv_sem.at[block, j],
            device_id=(me_r, target), device_id_type=MESH,
        )

    def arrived(block, j):
        hop(2, block, j).wait_recv()

    up, down = z < lines - 1, z > 0
    late = PIECES // 2

    def line_sends(block, j, act):
        @pl.when(up)
        def _():
            act(hop(0, block, j))

        @pl.when(down)
        def _():
            act(hop(1, block, j))

    own_load.wait()
    for j in range(PIECES):
        line_sends(me_c, j, lambda h: h.start())
        hop(2, me_c, j).start()

    ph_load.wait()

    def project(pair):
        acc[...] = jnp.zeros_like(acc)
        step = 2048

        def add(i, _):
            at = pl.ds(pl.multiple_of(i * step, step), step)
            lhs = jnp.concatenate([g[2 * pair, :, at], g[2 * pair + 1, :, at]], axis=0)
            acc[...] += jnp.dot(lhs, ph[at, :], preferred_element_type=jnp.float32)
            return 0

        lax.fori_loop(0, people // step, add, 0)
        part_f[...] = acc[...].T
        for s in range(sets):
            part[pair, s * t_here:(s + 1) * t_here, :] = part_f[pl.ds(s, t_here, stride=sets), :].astype(jnp.bfloat16)

        @pl.when(pair != me_r)
        def _():
            reduce_copy(pair).start()

    def lay(pair):
        step = 512
        lanes = pl.ds(pl.multiple_of(pair * LANES, LANES), LANES)

        def turn(i, _):
            at = pl.ds(pl.multiple_of(i * step, step), step)
            w_out[at, lanes] = jnp.concatenate([g[2 * pair, :, at], g[2 * pair + 1, :, at]], axis=0).T
            return 0

        lax.fori_loop(0, people // step, turn, 0)

    def reduce_copy(pair):
        return pltpu.make_async_remote_copy(
            src_ref=part.at[pair], dst_ref=rparts.at[me_r],
            send_sem=rs_send.at[pair], recv_sem=rs_recv.at[me_r],
            device_id=(pair, me_c), device_id_type=MESH,
        )

    def wait_theirs(pair):
        for j in range(PIECES):
            arrived(2 * pair + 1 - y, j)

    def around(s, fn):
        @pl.when(z - s >= 0)
        def _():
            fn(z - s)

        @pl.when(z + s < lines)
        def _():
            fn(z + s)

    def late_round(pair):
        wait_theirs(pair)
        project(pair)

    for s in range(1, lines):
        for j in range(PIECES):
            skip = s == 1 and j >= late

            @pl.when(z - s >= 0)
            def _():
                b = me_c - 2 * s
                arrived(b, j)

                @pl.when(up)
                def _():
                    hop(0, b, j).start()

                if not skip:
                    hop(2, b, j).start()

            @pl.when(z + s < lines)
            def _():
                b = me_c + 2 * s
                arrived(b, j)

                @pl.when(down)
                def _():
                    hop(1, b, j).start()

                if not skip:
                    hop(2, b, j).start()

        if s == 1:
            wait_theirs(z)
            project(z)
            lay(z)
    for j in range(late, PIECES):
        line_sends(other, j, lambda h: h.start())
    for s in range(2, lines - 1):
        around(s, late_round)
        around(s, lay)
    for s in (lines - 1, 1):
        around(s, late_round)
    around(lines - 1, lay)

    total = part[me_r].astype(jnp.float32)
    for d in range(1, rows):
        src = lax.rem(me_r + d, rows)
        pltpu.make_async_remote_copy(
            src_ref=part.at[src], dst_ref=rparts.at[src], send_sem=rs_send.at[src], recv_sem=rs_recv.at[src],
            device_id=(src, me_c), device_id_type=MESH,
        ).wait_recv()
        total = total + rparts[src].astype(jnp.float32)
    sb[...] = total.astype(jnp.bfloat16).reshape(sb.shape)

    def trade1(peer, slot):
        return pltpu.make_async_remote_copy(
            src_ref=sb.at[peer], dst_ref=rb.at[slot], send_sem=a1_send.at[peer], recv_sem=a1_recv.at[slot],
            device_id=(me_r, peer), device_id_type=MESH,
        )

    def trade2(peer, slot):
        return pltpu.make_async_remote_copy(
            src_ref=ob.at[peer], dst_ref=crow.at[me_r, slot], send_sem=a2_send.at[peer], recv_sem=a2_recv.at[slot],
            device_id=(me_r, peer), device_id_type=MESH,
        )

    def share(peer, slot):
        return pltpu.make_async_remote_copy(
            src_ref=crow.at[me_r], dst_ref=crow.at[slot], send_sem=ag_send.at[peer], recv_sem=ag_recv.at[slot],
            device_id=(peer, me_c), device_id_type=MESH,
        )

    col_peers = [lax.rem(me_c + d, cols) for d in range(1, cols)]
    row_peers = [lax.rem(me_r + d, rows) for d in range(1, rows)]
    for p in col_peers:
        trade1(p, me_c).start()
    rb[me_c] = sb[me_c]
    around(1, lay)
    product = kin[pl.ds(me_r, 1), :] * jnp.broadcast_to(trait[...], (LANES, traits)).T
    weight = product / (product + 1.0)
    for p in col_peers:
        trade1(p, p).wait_recv()
    s_here = sets // cols
    got = jnp.concatenate(
        [rb[:, s * t_here:(s + 1) * t_here, :].astype(jnp.float32).reshape(traits, LANES) for s in range(s_here)], axis=1
    )
    rotated = jnp.dot(basis[...].T, got, precision=HIGH, preferred_element_type=jnp.float32)
    scaled = rotated * jnp.concatenate([weight] * s_here, axis=1)
    back = jnp.dot(basis[...], scaled, precision=HIGH, preferred_element_type=jnp.float32)
    for s in range(s_here):
        ob[:, s * t_here:(s + 1) * t_here, :] = (
            back[:, s * LANES:(s + 1) * LANES].reshape(cols, t_here, LANES).astype(jnp.bfloat16)
        )
    for p in col_peers:
        trade2(p, me_c).start()
    crow[me_r, me_c] = ob[me_c]
    for p in col_peers:
        trade2(p, p).wait_recv()
    for p in row_peers:
        share(p, me_r).start()

    def place(r):
        for s in range(sets):
            part_s = crow[r, s // s_here, (s % s_here) * t_here:(s % s_here + 1) * t_here, :]
            ct[pl.ds(s, t_here, stride=sets), :] = part_s.astype(jnp.float32)
        turned = ct[...].T
        c_out[pl.ds(pl.multiple_of(r * LANES, LANES), LANES), :] = turned.astype(jnp.bfloat16)
        return turned

    coeffs_out[...] = place(me_r)
    for p in row_peers:
        share(p, p).wait_recv()
        place(p)

    tiles = gen_sem.shape[0]
    size = people // tiles

    def emit(i):
        at = pl.ds(pl.multiple_of(i * size, size), size)
        return pltpu.make_async_copy(held.at[at], gen_out.at[at], gen_sem.at[i])

    def predict(i, _):
        at = pl.ds(pl.multiple_of(i * size, size), size)
        held[at, :] = jnp.dot(w_out[at, :], c_out[...], preferred_element_type=jnp.float32).astype(jnp.bfloat16)
        emit(i).start()
        return 0

    lax.fori_loop(0, tiles, predict, 0)

    for j in range(PIECES):
        line_sends(me_c, j, lambda h: h.wait_send())
        hop(2, me_c, j).wait_send()
        if j >= late:
            line_sends(other, j, lambda h: h.wait_send())
        for s in range(1, lines):
            skip = s == 1 and j >= late

            @pl.when(z - s >= 0)
            def _():
                @pl.when(up)
                def _():
                    hop(0, me_c - 2 * s, j).wait_send()

                if not skip:
                    hop(2, me_c - 2 * s, j).wait_send()

            @pl.when(z + s < lines)
            def _():
                @pl.when(down)
                def _():
                    hop(1, me_c + 2 * s, j).wait_send()

                if not skip:
                    hop(2, me_c + 2 * s, j).wait_send()

    for p in row_peers:
        reduce_copy(p).wait_send()
        share(p, me_r).wait_send()
    for p in col_peers:
        trade1(p, me_c).wait_send()
        trade2(p, me_c).wait_send()

    def finish(i, _):
        emit(i).wait()
        return 0

    lax.fori_loop(0, tiles, finish, 0)


def fused(panel, pheno, kin_values, trait_values, trait_basis):
    rows, cols = lax.axis_size("row"), lax.axis_size("col")
    ind, columns = pheno.shape
    traits = trait_basis.shape[0]
    sets = columns * cols // traits
    share = kin_values.shape[0] // rows
    bf, f32 = jnp.bfloat16, jnp.float32
    hbm = pl.BlockSpec(memory_space=pltpu.HBM)
    vmem = pl.BlockSpec(memory_space=pltpu.VMEM)
    lot = columns // cols
    dma = pltpu.SemaphoreType.DMA
    genetic, coeffs = pl.pallas_call(
        functools.partial(gather_rotate, rows, cols),
        out_shape=(
            jax.ShapeDtypeStruct((ind, columns), bf),
            jax.ShapeDtypeStruct((share, columns), f32),
        ),
        in_specs=[hbm, hbm, vmem, vmem, vmem],
        out_specs=(hbm, vmem),
        scratch_shapes=[
            pltpu.VMEM((ind, rows * share), bf),
            pltpu.VMEM((rows * share, columns), bf),
            pltpu.VMEM((ind, columns), bf),
            dma((16,)),
            pltpu.VMEM((cols, panel.shape[1], ind), bf),
            pltpu.VMEM((ind, columns), bf),
            pltpu.VMEM((share, columns), f32),
            pltpu.VMEM((columns, LANES), f32),
            pltpu.VMEM((rows, columns, LANES), bf),
            pltpu.VMEM((rows, columns, LANES), bf),
            pltpu.VMEM((cols, lot, LANES), bf),
            pltpu.VMEM((cols, lot, LANES), bf),
            pltpu.VMEM((cols, lot, LANES), bf),
            pltpu.VMEM((rows, cols, lot, LANES), bf),
            pltpu.VMEM((columns, LANES), f32),
            dma((2,)), dma((3, cols, PIECES)), dma((cols, PIECES)),
            dma((rows,)), dma((rows,)), dma((cols,)), dma((cols,)), dma((cols,)), dma((cols,)),
            dma((rows,)), dma((rows,)),
        ],
        compiler_params=pltpu.CompilerParams(
            collective_id=0, has_side_effects=True, vmem_limit_bytes=48 * 1024 * 1024
        ),
    )(panel.T, pheno, trait_basis, kin_values.reshape(rows, share), trait_values[None, :])
    return coeffs, genetic


def local(panel, pheno, kin_values, trait_values, trait_basis):
    rows, cols = lax.axis_size("row"), lax.axis_size("col")
    eigen = kin_values.shape[0]
    if 2 * panel.shape[1] == LANES and eigen // rows == LANES and trait_basis.shape[0] // cols == 16:
        return fused(panel, pheno, kin_values, trait_values, trait_basis)
    return plain(panel, pheno, kin_values, trait_values, trait_basis)


def plain(panel, pheno, kin_values, trait_values, trait_basis):
    col_count = lax.axis_size("col")
    columns = pheno.shape[1]
    traits = trait_basis.shape[0]
    traits_here = traits // col_count
    set_count = columns // traits_here
    sets_dev = set_count // col_count
    whole_panel = lax.all_gather(panel, "col", axis=1, tiled=True)
    partial_value = lax.dot_general(
        whole_panel, pheno, (((0,), (0,)), ((), ())), preferred_element_type=jnp.float32
    )
    summed = lax.psum_scatter(partial_value, "row", scatter_dimension=0, tiled=True)
    first_row = lax.axis_index("row") * summed.shape[0]
    share_rows = summed.shape[0]
    by_trait = summed.reshape(share_rows, traits_here, set_count).transpose(0, 2, 1)
    by_trait = by_trait.reshape(share_rows, set_count * traits_here)
    grouped = lax.all_to_all(by_trait, "col", split_axis=1, concat_axis=1, tiled=True)
    grouped = grouped.reshape(share_rows, col_count, sets_dev, traits_here).transpose(0, 2, 1, 3)
    grouped = grouped.reshape(share_rows, sets_dev, traits)
    rotated = jnp.einsum("rst,tj->rsj", grouped, trait_basis, precision=HIGH)
    kin_rows = lax.dynamic_slice_in_dim(kin_values, first_row, share_rows, 0)
    product = kin_rows[:, None] * trait_values[None, :]
    scaled = rotated * (product / (product + 1.0))[:, None, :]
    unrotated = jnp.einsum("rsj,tj->rst", scaled, trait_basis, precision=HIGH)
    outgoing = unrotated.reshape(share_rows, sets_dev, col_count, traits_here).transpose(0, 2, 1, 3)
    outgoing = outgoing.reshape(share_rows, col_count * sets_dev * traits_here)
    returned = lax.all_to_all(outgoing, "col", split_axis=1, concat_axis=1, tiled=True)
    coeffs = returned.reshape(share_rows, set_count, traits_here).transpose(0, 2, 1)
    coeffs = coeffs.reshape(share_rows, columns)
    coeffs_low = lax.all_gather(coeffs.astype(jnp.bfloat16), "row", axis=0, tiled=True)
    genetic = jnp.dot(whole_panel, coeffs_low, preferred_element_type=jnp.float32)
    return (coeffs, genetic.astype(jnp.bfloat16))


def solution(mesh):
    return jax.shard_map(
        local,
        mesh=mesh,
        in_specs=(P("row", "col"), P("row", "col"), P(), P(), P()),
        out_specs=(P("row", "col"), P("row", "col")),
        check_vma=False,
    )
```

```python
import functools

import jax
import jax.numpy as jnp
from jax import lax
from jax.experimental import pallas as pl
from jax.experimental.pallas import tpu as pltpu
from jax.sharding import PartitionSpec as P

LANES = 128
PIECES = 4
MESH = pl.DeviceIdType.MESH
HIGH = lax.Precision.HIGHEST


def gather_rotate(
    rows, cols, q, pheno, basis_in, kin_in, trait_in,
    gen_out, coeffs_out,
    basis, kin, trait, w_out, c_out, held, gen_sem, g, ph, acc, part_f, part, rparts, sb, rb, ob, crow, ct,
    load_sem, send_sem, recv_sem, rs_send, rs_recv, a1_send, a1_recv, a2_send, a2_recv, ag_send, ag_recv,
):
    me_r, me_c = lax.axis_index("row"), lax.axis_index("col")
    lines = cols // 2
    z, y = me_c // 2, lax.rem(me_c, 2)
    other = me_c + 1 - 2 * y
    width, people = q.shape
    piece = people // PIECES
    columns = pheno.shape[1]
    traits = basis.shape[0]
    sets = columns * cols // traits
    t_here = traits // cols

    own_load = pltpu.make_async_copy(q, g.at[me_c], load_sem.at[0])
    own_load.start()
    ph_load = pltpu.make_async_copy(pheno, ph, load_sem.at[1])
    ph_load.start()
    small = [
        pltpu.make_async_copy(a, b, load_sem.at[2 + i])
        for i, (a, b) in enumerate(((basis_in, basis), (kin_in, kin), (trait_in, trait)))
    ]
    for copy in small:
        copy.start()

    barrier = pltpu.get_barrier_semaphore()
    for d in range(1, cols):
        pl.semaphore_signal(barrier, inc=1, device_id=(me_r, lax.rem(me_c + d, cols)), device_id_type=MESH)
    for d in range(1, rows):
        pl.semaphore_signal(barrier, inc=1, device_id=(lax.rem(me_r + d, rows), me_c), device_id_type=MESH)
    pl.semaphore_wait(barrier, cols + rows - 2)

    def hop(way, block, j):
        target = (jnp.minimum(me_c + 2, cols - 2 + y), jnp.maximum(me_c - 2, y), other)[way]
        here = g.at[block, :, pl.ds(j * piece, piece)]
        return pltpu.make_async_remote_copy(
            src_ref=here, dst_ref=here,
            send_sem=send_sem.at[way, block, j], recv_sem=recv_sem.at[block, j],
            device_id=(me_r, target), device_id_type=MESH,
        )

    def arrived(block, j):
        hop(2, block, j).wait_recv()

    up, down = z < lines - 1, z > 0
    late = PIECES // 2

    def line_sends(block, j, act):
        @pl.when(up)
        def _():
            act(hop(0, block, j))

        @pl.when(down)
        def _():
            act(hop(1, block, j))

    own_load.wait()
    for j in range(PIECES):
        line_sends(me_c, j, lambda h: h.start())
        hop(2, me_c, j).start()

    acc[...] = jnp.zeros_like(acc)
    ph_load.wait()

    def process(pair, j):
        arrived(2 * pair + 1 - y, j)
        lanes = pl.ds(pl.multiple_of(pair * LANES, LANES), LANES)
        at = pl.ds(j * piece, piece)
        lhs = jnp.concatenate([g[2 * pair, :, at], g[2 * pair + 1, :, at]], axis=0)
        acc[pair] += jnp.dot(lhs, ph[at, :], preferred_element_type=jnp.float32)
        w_out[at, lanes] = lhs.T

    def by_set(s):
        return part_f[pl.ds(s, t_here, stride=sets), :]

    def finish_pair(pair):
        @pl.when(pair != me_r)
        def _():
            part_f[...] = acc[pair].T
            for s in range(sets):
                part[pair, s * t_here:(s + 1) * t_here, :] = by_set(s).astype(jnp.bfloat16)
            reduce_copy(pair).start()

    def reduce_copy(pair):
        return pltpu.make_async_remote_copy(
            src_ref=part.at[pair], dst_ref=rparts.at[me_r],
            send_sem=rs_send.at[pair], recv_sem=rs_recv.at[me_r],
            device_id=(pair, me_c), device_id_type=MESH,
        )

    def around(s, fn):
        if s == 0:
            fn(z)
            return

        def side(i, _):
            pair = z - s + 2 * s * i

            @pl.when(jnp.logical_and(pair >= 0, pair < lines))
            def _():
                fn(pair)

            return 0

        lax.fori_loop(0, 2, side, 0)

    order = [(0, j) for j in range(PIECES)] + [(1, j) for j in range(late)]
    order += [(s, j) for s in range(2, lines) for j in range(PIECES)]
    tail = [(1, j) for j in range(late, PIECES)]
    done = 0

    def handle(s, j):
        around(s, lambda pair: process(pair, j))
        if j == PIECES - 1:
            around(s, finish_pair)

    for s in range(1, lines):
        for j in range(PIECES):
            skip = s == 1 and j >= late

            @pl.when(z - s >= 0)
            def _():
                b = me_c - 2 * s
                arrived(b, j)

                @pl.when(up)
                def _():
                    hop(0, b, j).start()

                if not skip:
                    hop(2, b, j).start()

            @pl.when(z + s < lines)
            def _():
                b = me_c + 2 * s
                arrived(b, j)

                @pl.when(down)
                def _():
                    hop(1, b, j).start()

                if not skip:
                    hop(2, b, j).start()

            if (s, j) != (1, 0):
                handle(*order[done])
                done += 1
    for j in range(late, PIECES):
        line_sends(other, j, lambda h: h.start())
    rest = order[done:]
    while rest or tail:
        if rest and len(rest) > len(tail):
            handle(*rest.pop(0))
        else:
            handle(*tail.pop(0))

    part_f[...] = acc[me_r].T
    total = jnp.concatenate([by_set(s) for s in range(sets)], axis=0)
    for d in range(1, rows):
        src = lax.rem(me_r + d, rows)
        pltpu.make_async_remote_copy(
            src_ref=part.at[src], dst_ref=rparts.at[src], send_sem=rs_send.at[src], recv_sem=rs_recv.at[src],
            device_id=(src, me_c), device_id_type=MESH,
        ).wait_recv()
        total = total + rparts[src].astype(jnp.float32)
    sb[...] = total.astype(jnp.bfloat16).reshape(sb.shape)

    def trade1(peer, slot):
        return pltpu.make_async_remote_copy(
            src_ref=sb.at[peer], dst_ref=rb.at[slot], send_sem=a1_send.at[peer], recv_sem=a1_recv.at[slot],
            device_id=(me_r, peer), device_id_type=MESH,
        )

    def trade2(peer, slot):
        return pltpu.make_async_remote_copy(
            src_ref=ob.at[peer], dst_ref=crow.at[me_r, slot], send_sem=a2_send.at[peer], recv_sem=a2_recv.at[slot],
            device_id=(me_r, peer), device_id_type=MESH,
        )

    def share(peer, slot):
        return pltpu.make_async_remote_copy(
            src_ref=crow.at[me_r], dst_ref=crow.at[slot], send_sem=ag_send.at[peer], recv_sem=ag_recv.at[slot],
            device_id=(peer, me_c), device_id_type=MESH,
        )

    col_peers = [lax.rem(me_c + d, cols) for d in range(1, cols)]
    row_peers = [lax.rem(me_r + d, rows) for d in range(1, rows)]
    for p in col_peers:
        trade1(p, me_c).start()
    rb[me_c] = sb[me_c]
    for copy in small:
        copy.wait()
    product = kin[pl.ds(me_r, 1), :] * jnp.broadcast_to(trait[...], (LANES, traits)).T
    weight = product / (product + 1.0)
    for p in col_peers:
        trade1(p, p).wait_recv()
    s_here = sets // cols
    got = jnp.concatenate(
        [rb[:, s * t_here:(s + 1) * t_here, :].astype(jnp.float32).reshape(traits, LANES) for s in range(s_here)], axis=1
    )
    rotated = jnp.dot(basis[...].T, got, precision=HIGH, preferred_element_type=jnp.float32)
    scaled = rotated * jnp.concatenate([weight] * s_here, axis=1)
    back = jnp.dot(basis[...], scaled, precision=HIGH, preferred_element_type=jnp.float32)
    for s in range(s_here):
        ob[:, s * t_here:(s + 1) * t_here, :] = (
            back[:, s * LANES:(s + 1) * LANES].reshape(cols, t_here, LANES).astype(jnp.bfloat16)
        )
    for p in col_peers:
        trade2(p, me_c).start()
    crow[me_r, me_c] = ob[me_c]
    for p in col_peers:
        trade2(p, p).wait_recv()
    for p in row_peers:
        share(p, me_r).start()

    def place(r):
        for s in range(sets):
            part_s = crow[r, s // s_here, (s % s_here) * t_here:(s % s_here + 1) * t_here, :]
            ct[pl.ds(s, t_here, stride=sets), :] = part_s.astype(jnp.float32)
        turned = ct[...].T
        c_out[pl.ds(pl.multiple_of(r * LANES, LANES), LANES), :] = turned.astype(jnp.bfloat16)
        return turned

    coeffs_out[...] = place(me_r)
    for p in row_peers:
        share(p, p).wait_recv()
        place(p)

    tiles = gen_sem.shape[0]
    size = people // tiles

    def emit(i):
        at = pl.ds(pl.multiple_of(i * size, size), size)
        return pltpu.make_async_copy(held.at[at], gen_out.at[at], gen_sem.at[i])

    def predict(i, _):
        at = pl.ds(pl.multiple_of(i * size, size), size)
        held[at, :] = jnp.dot(w_out[at, :], c_out[...], preferred_element_type=jnp.float32).astype(jnp.bfloat16)
        emit(i).start()
        return 0

    lax.fori_loop(0, tiles, predict, 0)

    for j in range(PIECES):
        line_sends(me_c, j, lambda h: h.wait_send())
        hop(2, me_c, j).wait_send()
        if j >= late:
            line_sends(other, j, lambda h: h.wait_send())
        for s in range(1, lines):
            skip = s == 1 and j >= late

            @pl.when(z - s >= 0)
            def _():
                @pl.when(up)
                def _():
                    hop(0, me_c - 2 * s, j).wait_send()

                if not skip:
                    hop(2, me_c - 2 * s, j).wait_send()

            @pl.when(z + s < lines)
            def _():
                @pl.when(down)
                def _():
                    hop(1, me_c + 2 * s, j).wait_send()

                if not skip:
                    hop(2, me_c + 2 * s, j).wait_send()

    for p in row_peers:
        reduce_copy(p).wait_send()
        share(p, me_r).wait_send()
    for p in col_peers:
        trade1(p, me_c).wait_send()
        trade2(p, me_c).wait_send()

    def finish(i, _):
        emit(i).wait()
        return 0

    lax.fori_loop(0, tiles, finish, 0)


def fused(panel, pheno, kin_values, trait_values, trait_basis):
    rows, cols = lax.axis_size("row"), lax.axis_size("col")
    ind, columns = pheno.shape
    traits = trait_basis.shape[0]
    sets = columns * cols // traits
    share = kin_values.shape[0] // rows
    bf, f32 = jnp.bfloat16, jnp.float32
    hbm = pl.BlockSpec(memory_space=pltpu.HBM)
    vmem = pl.BlockSpec(memory_space=pltpu.VMEM)
    lot = columns // cols
    dma = pltpu.SemaphoreType.DMA
    genetic, coeffs = pl.pallas_call(
        functools.partial(gather_rotate, rows, cols),
        out_shape=(
            jax.ShapeDtypeStruct((ind, columns), bf),
            jax.ShapeDtypeStruct((share, columns), f32),
        ),
        in_specs=[hbm] * 5,
        out_specs=(hbm, vmem),
        scratch_shapes=[
            pltpu.VMEM((traits, traits), f32),
            pltpu.VMEM((rows, share), f32),
            pltpu.VMEM((1, traits), f32),
            pltpu.VMEM((ind, rows * share), bf),
            pltpu.VMEM((rows * share, columns), bf),
            pltpu.VMEM((ind, columns), bf),
            dma((16,)),
            pltpu.VMEM((cols, panel.shape[1], ind), bf),
            pltpu.VMEM((ind, columns), bf),
            pltpu.VMEM((cols // 2, share, columns), f32),
            pltpu.VMEM((columns, LANES), f32),
            pltpu.VMEM((rows, columns, LANES), bf),
            pltpu.VMEM((rows, columns, LANES), bf),
            pltpu.VMEM((cols, lot, LANES), bf),
            pltpu.VMEM((cols, lot, LANES), bf),
            pltpu.VMEM((cols, lot, LANES), bf),
            pltpu.VMEM((rows, cols, lot, LANES), bf),
            pltpu.VMEM((columns, LANES), f32),
            dma((5,)), dma((3, cols, PIECES)), dma((cols, PIECES)),
            dma((rows,)), dma((rows,)), dma((cols,)), dma((cols,)), dma((cols,)), dma((cols,)),
            dma((rows,)), dma((rows,)),
        ],
        compiler_params=pltpu.CompilerParams(
            collective_id=0, has_side_effects=True, vmem_limit_bytes=56 * 1024 * 1024
        ),
    )(panel.T, pheno, trait_basis, kin_values.reshape(rows, share), trait_values[None, :])
    return coeffs, genetic


def local(panel, pheno, kin_values, trait_values, trait_basis):
    rows, cols = lax.axis_size("row"), lax.axis_size("col")
    eigen = kin_values.shape[0]
    if 2 * panel.shape[1] == LANES and eigen // rows == LANES and trait_basis.shape[0] // cols == 16:
        return fused(panel, pheno, kin_values, trait_values, trait_basis)
    return plain(panel, pheno, kin_values, trait_values, trait_basis)


def plain(panel, pheno, kin_values, trait_values, trait_basis):
    col_count = lax.axis_size("col")
    columns = pheno.shape[1]
    traits = trait_basis.shape[0]
    traits_here = traits // col_count
    set_count = columns // traits_here
    sets_dev = set_count // col_count
    whole_panel = lax.all_gather(panel, "col", axis=1, tiled=True)
    partial_value = lax.dot_general(
        whole_panel, pheno, (((0,), (0,)), ((), ())), preferred_element_type=jnp.float32
    )
    summed = lax.psum_scatter(partial_value, "row", scatter_dimension=0, tiled=True)
    first_row = lax.axis_index("row") * summed.shape[0]
    share_rows = summed.shape[0]
    by_trait = summed.reshape(share_rows, traits_here, set_count).transpose(0, 2, 1)
    by_trait = by_trait.reshape(share_rows, set_count * traits_here)
    grouped = lax.all_to_all(by_trait, "col", split_axis=1, concat_axis=1, tiled=True)
    grouped = grouped.reshape(share_rows, col_count, sets_dev, traits_here).transpose(0, 2, 1, 3)
    grouped = grouped.reshape(share_rows, sets_dev, traits)
    rotated = jnp.einsum("rst,tj->rsj", grouped, trait_basis, precision=HIGH)
    kin_rows = lax.dynamic_slice_in_dim(kin_values, first_row, share_rows, 0)
    product = kin_rows[:, None] * trait_values[None, :]
    scaled = rotated * (product / (product + 1.0))[:, None, :]
    unrotated = jnp.einsum("rsj,tj->rst", scaled, trait_basis, precision=HIGH)
    outgoing = unrotated.reshape(share_rows, sets_dev, col_count, traits_here).transpose(0, 2, 1, 3)
    outgoing = outgoing.reshape(share_rows, col_count * sets_dev * traits_here)
    returned = lax.all_to_all(outgoing, "col", split_axis=1, concat_axis=1, tiled=True)
    coeffs = returned.reshape(share_rows, set_count, traits_here).transpose(0, 2, 1)
    coeffs = coeffs.reshape(share_rows, columns)
    coeffs_low = lax.all_gather(coeffs.astype(jnp.bfloat16), "row", axis=0, tiled=True)
    genetic = jnp.dot(whole_panel, coeffs_low, preferred_element_type=jnp.float32)
    return (coeffs, genetic.astype(jnp.bfloat16))


def solution(mesh):
    return jax.shard_map(
        local,
        mesh=mesh,
        in_specs=(P("row", "col"), P("row", "col"), P(), P(), P()),
        out_specs=(P("row", "col"), P("row", "col")),
        check_vma=False,
    )
```
